8 devices in a mesh: dp: 2 (over y, z), tp: 4 (over x, core).
Axes of the slice: x: 2, y: 2, z: 1, core: 2. Of those that a mesh axis runs over, the one named last changes fastest.
Arguments:
- x: bfloat16 [1280, 6656], P(('dp', 'tp')), parts along dimension 0
- w_gate: bfloat16 [6656, 17920], P(None, 'tp')
- w_up: bfloat16 [6656, 17920], P(None, 'tp')
- w_down: bfloat16 [17920, 6656], P('tp')
Outputs:
- output: bfloat16 [1280, 6656], P(('dp', 'tp')), parts along dimension 0
There are 2 independent parts. The reference program is written for one: setup_inputs(seed, part) draws one part's arguments, and reference() takes and returns one part's arrays. A program takes and returns all parts, laid end to end along the dimension named above; an argument that names none is the same for every part.
All inputs are finite; a program needn't handle non-finite values.
Results may differ from the reference program's by a relative error of at most 0.016.
Values are sent between devices in bfloat16 or wider.
A program may use at most 2 GiB of HBM per device.

```python
import jax
import jax.numpy as jnp

ROWS = 640
D = 6656
FF = 17920


def setup_inputs(seed: int = 0, part: int = 0) -> dict:
    kx, kg, ku, kd = jax.random.split(jax.random.key(seed), 4)
    drawn = {
        "x": jax.random.normal(jax.random.fold_in(kx, part), (ROWS, D), jnp.float32),
        "w_gate": jax.random.normal(kg, (D, FF), jnp.float32) * D**-0.5,
        "w_up": jax.random.normal(ku, (D, FF), jnp.float32) * D**-0.5,
        "w_down": jax.random.normal(kd, (FF, D), jnp.float32) * FF**-0.5,
    }
    return {k: v.astype(jnp.bfloat16) for k, v in drawn.items()}


def reference(x, w_gate, w_up, w_down):
    gate = jnp.dot(x, w_gate, preferred_element_type=jnp.float32)
    up = jnp.dot(x, w_up, preferred_element_type=jnp.float32)
    hidden = (jax.nn.silu(gate) * up).astype(jnp.bfloat16)
    return jnp.dot(hidden, w_down, preferred_element_type=jnp.float32).astype(jnp.bfloat16)
```

```python
import functools

import jax
import jax.numpy as jnp
from jax import lax
from jax.experimental import pallas as pl
from jax.experimental.pallas import tpu as pltpu
from jax.sharding import PartitionSpec as P

MESH = pl.DeviceIdType.MESH
F32 = jnp.float32
BF16 = jnp.bfloat16

D = 6656
FF = 4480
ROWS = 160
NT = 256
NFULL = FF // NT
TAIL = FF - NFULL * NT
CW = 512
NC = D // CW
SLOTS = 3


def kernel(
    x_ref, wg_ref, wu_ref, wd_ref, y_ref,
    xall, hid, wbuf, wdbuf,
    kept, send_r, recv_r, stage, recv_x, send_l, recv_l, acc_l,
    xsem, wsem, wdsem, tailsem,
    ag_send, ag_recv, fw_send, fw_recv, px_send, px_recv,
    rr_send, rr_recv, rx_send, rx_recv, rl_send, rl_recv, ysem,
):
    dp = lax.axis_index("dp")
    tp = lax.axis_index("tp")
    core = lax.rem(tp, 2)
    chip = lax.div(tp, 2)
    partner = (dp, chip * 2 + (1 - core))
    remote = (dp, (1 - chip) * 2 + core)

    def gate_up_copies(step, slot):
        col = pl.ds(pl.multiple_of(lax.rem(step, NFULL) * NT, NT), NT)
        return [
            pltpu.make_async_copy(w.at[:, col], wbuf.at[slot, j], wsem.at[slot, j])
            for j, w in enumerate((wg_ref, wu_ref))
        ]

    def down_copy(n, slot):
        col = pl.ds(pl.multiple_of(n * CW, CW), CW)
        return pltpu.make_async_copy(wd_ref.at[:, col], wdbuf.at[slot], wdsem.at[slot])

    def tail_copies():
        slot = (2 * NFULL) % SLOTS
        return [
            pltpu.make_async_copy(
                w.at[:, pl.ds(NFULL * NT, TAIL)],
                wbuf.at[slot, 0, :, pl.ds(j * TAIL, TAIL)],
                tailsem.at[j],
            )
            for j, w in enumerate((wg_ref, wu_ref))
        ]

    own = pltpu.make_async_copy(x_ref, xall.at[pl.ds(0, ROWS)], xsem)
    own.start()
    for s in range(SLOTS - 1):
        for c in gate_up_copies(s, s):
            c.start()

    barrier = pltpu.get_barrier_semaphore()
    for other in (partner, remote):
        pl.semaphore_signal(barrier, inc=1, device_id=other, device_id_type=MESH)
    pl.semaphore_wait(barrier, 2)

    to_partner = pltpu.make_async_remote_copy(
        src_ref=x_ref, dst_ref=xall.at[pl.ds(ROWS, ROWS)],
        send_sem=px_send, recv_sem=px_recv,
        device_id=partner, device_id_type=MESH,
    )
    to_partner.start()

    def chunk(c):
        return pl.ds(pl.multiple_of(c * CW, CW), CW)

    def gather_copy(c):
        return pltpu.make_async_remote_copy(
            src_ref=x_ref.at[:, chunk(c)],
            dst_ref=xall.at[pl.ds(2 * ROWS, ROWS), chunk(c)],
            send_sem=ag_send.at[c], recv_sem=ag_recv.at[c],
            device_id=remote, device_id_type=MESH,
        )

    def forward_copy(c):
        return pltpu.make_async_remote_copy(
            src_ref=xall.at[pl.ds(2 * ROWS, ROWS), chunk(c)],
            dst_ref=xall.at[pl.ds(3 * ROWS, ROWS), chunk(c)],
            send_sem=fw_send.at[c], recv_sem=fw_recv.at[c],
            device_id=partner, device_id_type=MESH,
        )

    @pl.loop(0, NC)
    def _(c):
        gather_copy(c).start()

    own.wait()
    to_partner.wait_recv()

    def forward(c):
        gather_copy(c).wait_recv()
        forward_copy(c).start()

    def gate_up(rows, step):
        slot = lax.rem(step, SLOTS)
        for c in gate_up_copies(step, slot):
            c.wait()
        ahead = step + SLOTS - 1

        @pl.when(ahead < 2 * NFULL)
        def _():
            for c in gate_up_copies(ahead, lax.rem(ahead, SLOTS)):
                c.start()

        g = jnp.dot(xall[rows], wbuf[slot, 0], preferred_element_type=F32)
        u = jnp.dot(xall[rows], wbuf[slot, 1], preferred_element_type=F32)
        col = pl.ds(pl.multiple_of(lax.rem(step, NFULL) * NT, NT), NT)
        hid[rows, col] = (jax.nn.silu(g) * u).astype(BF16)

    @pl.loop(0, NFULL)
    def _(i):
        gate_up(pl.ds(0, 2 * ROWS), i)
        lo = lax.div(2 * i, 3)
        hi = lax.div(2 * i + 2, 3)

        @pl.when(hi > lo)
        def _():
            forward(lo)

    for c in range((2 * NFULL) // 3, NC):
        forward(c)
    for c in range(NC):
        forward_copy(c).wait_recv()

    @pl.loop(0, NFULL)
    def _(i):
        gate_up(pl.ds(2 * ROWS, 2 * ROWS), NFULL + i)

        @pl.when(i == NFULL - 2)
        def _():
            for c in tail_copies():
                c.start()

        @pl.when(i == NFULL - 1)
        def _():
            for n in range(2):
                down_copy(n, n).start()

    for c in tail_copies():
        c.wait()
    for r in (pl.ds(2 * ROWS, 2 * ROWS), pl.ds(0, 2 * ROWS)):
        gu = jnp.dot(xall[r], wbuf[(2 * NFULL) % SLOTS, 0], preferred_element_type=F32)
        hid[r, pl.ds(NFULL * NT, TAIL)] = (
            jax.nn.silu(gu[:, :TAIL]) * gu[:, TAIL:]
        ).astype(BF16)

    def side_copy(src, dst, n, ssem, rsem, dev):
        return pltpu.make_async_remote_copy(
            src_ref=src, dst_ref=dst.at[n], send_sem=ssem.at[n], recv_sem=rsem.at[n],
            device_id=dev, device_id_type=MESH,
        )

    def r_copy(n):
        return side_copy(send_r.at[lax.rem(n, 2)], recv_r, n, rr_send, rr_recv, partner)

    def l_copy(n):
        return side_copy(send_l.at[lax.rem(n, 2)], recv_l, n, rl_send, rl_recv, partner)

    def x_copy(n):
        return side_copy(stage.at[n], recv_x, n, rx_send, rx_recv, remote)

    @pl.loop(0, NC)
    def _(n):
        slot = lax.rem(n, 2)
        down_copy(n, slot).wait()

        @pl.when(n >= 2)
        def _():
            r_copy(n - 2).wait_send()
            l_copy(n - 2).wait_send()

        pr = jnp.dot(hid[pl.ds(2 * ROWS, 2 * ROWS)], wdbuf[slot], preferred_element_type=F32)
        kept[...] = pr[:ROWS]
        send_r[slot] = pr[ROWS:].astype(BF16)
        r_copy(n).start()
        pll = jnp.dot(hid[pl.ds(0, 2 * ROWS)], wdbuf[slot], preferred_element_type=F32)
        acc_l[n] = pll[:ROWS]
        send_l[slot] = pll[ROWS:].astype(BF16)
        l_copy(n).start()

        @pl.when(n + 2 < NC)
        def _():
            down_copy(n + 2, slot).start()

        r_copy(n).wait_recv()
        stage[n] = (kept[...] + recv_r[n].astype(F32)).astype(BF16)
        x_copy(n).start()

    def y_copy(n):
        return pltpu.make_async_copy(stage.at[n], y_ref.at[:, chunk(n)], ysem.at[n])

    @pl.loop(0, NC)
    def _(n):
        l_copy(n).wait_recv()
        x_copy(n).wait()
        total = acc_l[n] + recv_l[n].astype(F32) + recv_x[n].astype(F32)
        stage[n] = total.astype(BF16)
        y_copy(n).start()

    for n in (NC - 2, NC - 1):
        r_copy(n).wait_send()
        l_copy(n).wait_send()
    to_partner.wait_send()

    @pl.loop(0, NC)
    def _(c):
        gather_copy(c).wait_send()
        forward_copy(c).wait_send()
        y_copy(c).wait()


def solution(mesh):
    dma = pltpu.SemaphoreType.DMA

    def step(x, w_gate, w_up, w_down):
        return pl.pallas_call(
            kernel,
            out_shape=jax.ShapeDtypeStruct((ROWS, D), BF16),
            in_specs=[pl.BlockSpec(memory_space=pl.ANY)] * 4,
            out_specs=pl.BlockSpec(memory_space=pl.ANY),
            scratch_shapes=[
                pltpu.VMEM((4 * ROWS, D), BF16),
                pltpu.VMEM((4 * ROWS, FF), BF16),
                pltpu.VMEM((SLOTS, 2, D, NT), BF16),
                pltpu.VMEM((2, FF, CW), BF16),
                pltpu.VMEM((ROWS, CW), F32),
                pltpu.VMEM((2, ROWS, CW), BF16),
                pltpu.VMEM((NC, ROWS, CW), BF16),
                pltpu.VMEM((NC, ROWS, CW), BF16),
                pltpu.VMEM((NC, ROWS, CW), BF16),
                pltpu.VMEM((2, ROWS, CW), BF16),
                pltpu.VMEM((NC, ROWS, CW), BF16),
                pltpu.VMEM((NC, ROWS, CW), F32),
                dma, dma((SLOTS, 2)), dma((2,)), dma((2,)),
                dma((NC,)), dma((NC,)), dma((NC,)), dma((NC,)), dma, dma,
                dma((NC,)), dma((NC,)), dma((NC,)), dma((NC,)), dma((NC,)), dma((NC,)),
                dma((NC,)),
            ],
            compiler_params=pltpu.CompilerParams(
                collective_id=0, has_side_effects=True, vmem_limit_bytes=67043328
            ),
            cost_estimate=pl.CostEstimate(
                flops=6 * 4 * ROWS * D * FF, bytes_accessed=3 * D * FF * 2, transcendentals=4 * ROWS * FF
            ),
        )(x, w_gate, w_up, w_down)

    return jax.shard_map(
        step,
        mesh=mesh,
        in_specs=(P(("dp", "tp"), None), P(None, "tp"), P(None, "tp"), P("tp", None)),
        out_specs=P(("dp", "tp"), None),
        check_vma=False,
    )
```

```python
import functools

import jax
import jax.numpy as jnp
from jax import lax
from jax.experimental import pallas as pl
from jax.experimental.pallas import tpu as pltpu
from jax.sharding import PartitionSpec as P

MESH = pl.DeviceIdType.MESH
F32 = jnp.float32
BF16 = jnp.bfloat16

D = 6656
FF = 4480
ROWS = 160
NT = 256
NFULL = FF // NT
TAIL = FF - NFULL * NT
CW = 512
NC = D // CW
SLOTS = 3
HALF = D // 2
PAIRS = NFULL // 2
EARLY = 12
LATE = NFULL - EARLY


def kernel(
    x_ref, wg_ref, wu_ref, wd_ref, y_ref,
    xall, hid, wbuf, acc,
    kept, send_r, recv_r, stage, recv_x, send_l, recv_l, acc_l,
    xsem, wsem,
    ag_send, ag_recv, fw_send, fw_recv, px_send, px_recv,
    rr_send, rr_recv, rx_send, rx_recv, rl_send, rl_recv, ysem,
):
    dp = lax.axis_index("dp")
    tp = lax.axis_index("tp")
    core = lax.rem(tp, 2)
    chip = lax.div(tp, 2)
    partner = (dp, chip * 2 + (1 - core))
    remote = (dp, (1 - chip) * 2 + core)

    def copies(parts, slot):
        return [
            pltpu.make_async_copy(src, wbuf.at[slot, j, pl.ds(row, src.shape[0]), pl.ds(c, src.shape[1])], wsem.at[slot, k])
            for k, (src, j, row, c) in enumerate(parts)
        ]

    def cols(ref, t):
        return ref.at[:, pl.ds(pl.multiple_of(t * NT, NT), NT)]

    def full(t, slot):
        return copies([(cols(w, t), j, 0, 0) for j, w in enumerate((wg_ref, wu_ref))], slot)

    def half(t, h, slot, tiles=2):
        return copies(
            [
                (cols(w.at[pl.ds(h * HALF, HALF)], t + q), j, q * HALF, 0)
                for q in range(tiles)
                for j, w in enumerate((wg_ref, wu_ref))
            ],
            slot,
        )

    def tail(slot):
        col = pl.ds(NFULL * NT, TAIL)
        return copies([(w.at[:, col], 0, 0, j * TAIL) for j, w in enumerate((wg_ref, wu_ref))], slot)

    def down(n, slot):
        return copies([(cols(wd_ref, 2 * n + j), j, 0, 0) for j in range(2)], slot)

    def start(cs):
        for c in cs:
            c.start()

    def wait(cs):
        for c in cs:
            c.wait()

    def slot_of(step):
        return lax.rem(step, SLOTS)

    own = pltpu.make_async_copy(x_ref, xall.at[pl.ds(0, ROWS)], xsem)
    own.start()
    for s in range(SLOTS - 1):
        start(full(s, s))

    barrier = pltpu.get_barrier_semaphore()
    for other in (partner, remote):
        pl.semaphore_signal(barrier, inc=1, device_id=other, device_id_type=MESH)
    pl.semaphore_wait(barrier, 2)

    to_partner = pltpu.make_async_remote_copy(
        src_ref=x_ref, dst_ref=xall.at[pl.ds(ROWS, ROWS)],
        send_sem=px_send, recv_sem=px_recv,
        device_id=partner, device_id_type=MESH,
    )
    to_partner.start()

    def chunk(c):
        return pl.ds(pl.multiple_of(c * CW, CW), CW)

    def gather_copy(c):
        return pltpu.make_async_remote_copy(
            src_ref=x_ref.at[:, chunk(c)],
            dst_ref=xall.at[pl.ds(2 * ROWS, ROWS), chunk(c)],
            send_sem=ag_send.at[c], recv_sem=ag_recv.at[c],
            device_id=remote, device_id_type=MESH,
        )

    def forward_copy(c):
        return pltpu.make_async_remote_copy(
            src_ref=xall.at[pl.ds(2 * ROWS, ROWS), chunk(c)],
            dst_ref=xall.at[pl.ds(3 * ROWS, ROWS), chunk(c)],
            send_sem=fw_send.at[c], recv_sem=fw_recv.at[c],
            device_id=partner, device_id_type=MESH,
        )

    @pl.loop(0, NC)
    def _(c):
        gather_copy(c).start()

    own.wait()
    to_partner.wait_recv()

    def forward(c):
        gather_copy(c).wait_recv()
        forward_copy(c).start()

    own_rows, far_rows = pl.ds(0, 2 * ROWS), pl.ds(2 * ROWS, 2 * ROWS)

    def dot(rows, ks, slot, j, at):
        return jnp.dot(
            xall[rows, ks], wbuf[slot, j, pl.ds(at, ks.size)], preferred_element_type=F32
        )

    def put(rows, t, g, u):
        hid[rows, pl.ds(pl.multiple_of(t * NT, NT), NT)] = (jax.nn.silu(g) * u).astype(BF16)

    def gate_up_own(t, slot):
        g, u = (dot(own_rows, pl.ds(0, D), slot, j, 0) for j in range(2))
        put(own_rows, t, g, u)

    def first_half(t, slot, tiles=2):
        for q in range(tiles):
            for j in range(2):
                acc[t + q, j] = dot(far_rows, pl.ds(0, HALF), slot, j, q * HALF)

    def second_half(t, slot, tiles=2):
        for q in range(tiles):
            g, u = (acc[t + q, j] + dot(far_rows, pl.ds(HALF, HALF), slot, j, q * HALF) for j in range(2))
            put(far_rows, t + q, g, u)

    def forward_at(i):
        lo = lax.div(2 * i, 3)

        @pl.when(lax.div(2 * i + 2, 3) > lo)
        def _():
            forward(lo)

    @pl.loop(0, EARLY)
    def _(i):
        slot, later = slot_of(i), slot_of(i + 2)
        wait(full(i, slot))

        @pl.when(i + 2 < EARLY)
        def _():
            start(full(i + 2, later))

        @pl.when(i + 2 >= EARLY)
        def _():
            start(half(2 * (i + 2 - EARLY), 0, later))

        gate_up_own(i, slot)
        forward_at(i)

    for c in range(7):
        forward_copy(c).wait_recv()

    S1 = EARLY

    @pl.loop(0, PAIRS)
    def _(p):
        slot, later = slot_of(S1 + p), slot_of(S1 + p + 2)
        wait(half(2 * p, 0, slot))

        @pl.when(p + 2 < PAIRS)
        def _():
            start(half(2 * p + 4, 0, later))

        @pl.when(p + 2 == PAIRS)
        def _():
            start(half(2 * PAIRS, 0, later, 1))

        @pl.when(p + 2 > PAIRS)
        def _():
            start(half(0, 1, later))

        first_half(2 * p, slot)
        forward_at(S1 + p)

    S2 = S1 + PAIRS
    wait(half(2 * PAIRS, 0, S2 % SLOTS, 1))
    start(half(2, 1, (S2 + 2) % SLOTS))
    first_half(2 * PAIRS, S2 % SLOTS, 1)
    for c in range(7, NC):
        forward_copy(c).wait_recv()

    S3 = S2 + 1

    @pl.loop(0, PAIRS)
    def _(p):
        slot, later = slot_of(S3 + p), slot_of(S3 + p + 2)
        wait(half(2 * p, 1, slot))

        @pl.when(p + 2 < PAIRS)
        def _():
            start(half(2 * p + 4, 1, later))

        @pl.when(p + 2 == PAIRS)
        def _():
            start(half(2 * PAIRS, 1, later, 1))

        @pl.when(p + 2 > PAIRS)
        def _():
            start(tail(later))

        second_half(2 * p, slot)

    S4 = S3 + PAIRS
    wait(half(2 * PAIRS, 1, S4 % SLOTS, 1))
    wait(tail((S4 + 1) % SLOTS))
    start(down(0, (S4 + 2) % SLOTS))
    second_half(2 * PAIRS, S4 % SLOTS, 1)
    for r in (far_rows, own_rows):
        gu = dot(r, pl.ds(0, D), (S4 + 1) % SLOTS, 0, 0)
        hid[r, pl.ds(NFULL * NT, TAIL)] = (
            jax.nn.silu(gu[:, :TAIL]) * gu[:, TAIL:]
        ).astype(BF16)
    S5 = S4 + 2
    start(full(EARLY, (S5 + 1) % SLOTS))

    def side_copy(src, dst, n, ssem, rsem, dev):
        return pltpu.make_async_remote_copy(
            src_ref=src, dst_ref=dst.at[n], send_sem=ssem.at[n], recv_sem=rsem.at[n],
            device_id=dev, device_id_type=MESH,
        )

    def r_copy(n):
        return side_copy(send_r.at[lax.rem(n, 2)], recv_r, n, rr_send, rr_recv, partner)

    def l_copy(n):
        m = lax.rem(n + NC - LATE, NC)
        return side_copy(send_l.at[lax.rem(m, 2)], recv_l, n, rl_send, rl_recv, partner)

    def x_copy(n):
        return side_copy(stage.at[n], recv_x, n, rx_send, rx_recv, remote)

    def term(rows, slot, j):
        return jnp.dot(hid[rows], wbuf[slot, j, pl.ds(0, FF)], preferred_element_type=F32)

    def down_far(n, slot):
        @pl.when(n >= 2)
        def _():
            r_copy(n - 2).wait_send()

        out = lax.rem(n, 2)
        for j in range(2):
            col = pl.ds(j * NT, NT)
            t = term(far_rows, slot, j)
            kept[:, col] = t[:ROWS]
            send_r[out, :, col] = t[ROWS:].astype(BF16)
        r_copy(n).start()

    def down_own(n, slot):
        m = lax.rem(n + NC - LATE, NC)

        @pl.when(m >= 2)
        def _():
            l_copy(lax.rem(n + NC - 2, NC)).wait_send()

        out = lax.rem(m, 2)
        for j in range(2):
            col = pl.ds(j * NT, NT)
            t = term(own_rows, slot, j)
            acc_l[n, :, col] = t[:ROWS]
            send_l[out, :, col] = t[ROWS:].astype(BF16)
        l_copy(n).start()

    def reduce_far(n):
        r_copy(n).wait_recv()
        stage[n] = (kept[...] + recv_r[n].astype(F32)).astype(BF16)
        x_copy(n).start()

    @pl.loop(0, LATE)
    def _(k):
        slot = slot_of(S5 + 2 * k)
        wait(down(k, slot))
        start(down(k + 1, slot_of(S5 + 2 * k + 2)))
        down_far(k, slot)
        slot = slot_of(S5 + 2 * k + 1)
        wait(full(EARLY + k, slot))

        @pl.when(k + 1 < LATE)
        def _():
            start(full(EARLY + k + 1, slot_of(S5 + 2 * k + 3)))

        @pl.when(k + 1 == LATE)
        def _():
            start(down(LATE + 1, slot_of(S5 + 2 * k + 3)))

        gate_up_own(EARLY + k, slot)
        reduce_far(k)

    S6 = S5 + 2 * LATE

    @pl.loop(LATE, NC)
    def _(n):
        slot = slot_of(S6 + n - LATE)
        wait(down(n, slot))
        start(down(lax.rem(n + 2, NC), slot_of(S6 + n - LATE + 2)))
        down_far(n, slot)
        down_own(n, slot)
        reduce_far(n)

    S7 = S6 + NC - LATE

    @pl.loop(0, LATE)
    def _(n):
        slot = slot_of(S7 + n)
        wait(down(n, slot))

        @pl.when(n + 2 < LATE)
        def _():
            start(down(n + 2, slot_of(S7 + n + 2)))

        down_own(n, slot)

    def y_copy(n):
        return pltpu.make_async_copy(stage.at[n], y_ref.at[:, chunk(n)], ysem.at[n])

    @pl.loop(0, NC)
    def _(n):
        l_copy(n).wait_recv()
        x_copy(n).wait()
        total = acc_l[n] + recv_l[n].astype(F32) + recv_x[n].astype(F32)
        stage[n] = total.astype(BF16)
        y_copy(n).start()

    for n in (NC - 2, NC - 1):
        r_copy(n).wait_send()
        l_copy((n + LATE) % NC).wait_send()
    to_partner.wait_send()

    @pl.loop(0, NC)
    def _(c):
        gather_copy(c).wait_send()
        forward_copy(c).wait_send()
        y_copy(c).wait()


def solution(mesh):
    dma = pltpu.SemaphoreType.DMA

    def step(x, w_gate, w_up, w_down):
        return pl.pallas_call(
            kernel,
            out_shape=jax.ShapeDtypeStruct((ROWS, D), BF16),
            in_specs=[pl.BlockSpec(memory_space=pl.ANY)] * 4,
            out_specs=pl.BlockSpec(memory_space=pl.ANY),
            scratch_shapes=[
                pltpu.VMEM((4 * ROWS, D), BF16),
                pltpu.VMEM((4 * ROWS, FF), BF16),
                pltpu.VMEM((SLOTS, 2, D, NT), BF16),
                pltpu.VMEM((NFULL, 2, 2 * ROWS, NT), F32),
                pltpu.VMEM((ROWS, CW), F32),
                pltpu.VMEM((2, ROWS, CW), BF16),
                pltpu.VMEM((NC, ROWS, CW), BF16),
                pltpu.VMEM((NC, ROWS, CW), BF16),
                pltpu.VMEM((NC, ROWS, CW), BF16),
                pltpu.VMEM((2, ROWS, CW), BF16),
                pltpu.VMEM((NC, ROWS, CW), BF16),
                pltpu.VMEM((NC, ROWS, CW), F32),
                dma, dma((SLOTS, 4)),
                dma((NC,)), dma((NC,)), dma((NC,)), dma((NC,)), dma, dma,
                dma((NC,)), dma((NC,)), dma((NC,)), dma((NC,)), dma((NC,)), dma((NC,)),
                dma((NC,)),
            ],
            compiler_params=pltpu.CompilerParams(
                collective_id=0, has_side_effects=True, vmem_limit_bytes=67043328
            ),
            cost_estimate=pl.CostEstimate(
                flops=6 * 4 * ROWS * D * FF, bytes_accessed=3 * D * FF * 2, transcendentals=4 * ROWS * FF
            ),
        )(x, w_gate, w_up, w_down)

    return jax.shard_map(
        step,
        mesh=mesh,
        in_specs=(P(("dp", "tp"), None), P(None, "tp"), P(None, "tp"), P("tp", None)),
        out_specs=P(("dp", "tp"), None),
        check_vma=False,
    )
```

```python
import functools

import jax
import jax.numpy as jnp
from jax import lax
from jax.experimental import pallas as pl
from jax.experimental.pallas import tpu as pltpu
from jax.sharding import PartitionSpec as P

MESH = pl.DeviceIdType.MESH
F32 = jnp.float32
BF16 = jnp.bfloat16

D = 6656
FF = 4480
ROWS = 160
NT = 256
NFULL = FF // NT
TAIL = FF - NFULL * NT
CW = 512
NC = D // CW
NX = D // NT
SLOTS = 4
HALF = D // 2
PAIRS = NFULL // 2
EARLY = 12
LATE = NFULL - EARLY - 1
S1 = EARLY
S2 = S1 + PAIRS
S3 = S2 + 2
S4 = S3 + PAIRS
S5 = S4 + 2


def kernel(
    x_ref, wg_ref, wu_ref, wd_ref, y_ref,
    xall, hid, wbuf, acc,
    kept, send_r, recv_r, stage, recv_x, send_l, recv_l,
    xsem, wsem,
    ag_send, ag_recv, fw_send, fw_recv, px_send, px_recv,
    rr_send, rr_recv, rx_send, rx_recv, rl_send, rl_recv, ysem,
):
    dp = lax.axis_index("dp")
    tp = lax.axis_index("tp")
    core = lax.rem(tp, 2)
    chip = lax.div(tp, 2)
    partner = (dp, chip * 2 + (1 - core))
    remote = (dp, (1 - chip) * 2 + core)

    def copies(parts, slot):
        return [
            pltpu.make_async_copy(src, wbuf.at[slot, j, pl.ds(row, src.shape[0]), pl.ds(c, src.shape[1])], wsem.at[slot, k])
            for k, (src, j, row, c) in enumerate(parts)
        ]

    def cols(ref, t):
        return ref.at[:, pl.ds(pl.multiple_of(t * NT, NT), NT)]

    def halves(pick, slot):
        parts = []
        for q in range(2):
            h, t = pick(q)
            row = pl.ds(pl.multiple_of(h * HALF, HALF), HALF)
            parts += [(cols(w.at[row], t), j, q * HALF, 0) for j, w in enumerate((wg_ref, wu_ref))]
        return copies(parts, slot)

    def full(t, slot):
        return halves(lambda q: (q, t), slot)

    def fetch(step):
        def pick(q):
            own = (step < S1) | (step == S3 - 1)
            p = step - jnp.where(step >= S3, S3, S1)
            h = jnp.where(own, q, jnp.where(step >= S3, 1, 0))
            t = jnp.where(own, jnp.minimum(step, EARLY), jnp.minimum(2 * p + q, NFULL - 1))
            return h, t

        return halves(pick, slot_of(step))

    def tail(slot):
        col = pl.ds(NFULL * NT, TAIL)
        return copies([(w.at[:, col], 0, 0, j * TAIL) for j, w in enumerate((wg_ref, wu_ref))], slot)

    def down(n, slot):
        return copies([(cols(wd_ref, 2 * n + j), j, 0, 0) for j in range(2)], slot)

    def start(cs):
        for c in cs:
            c.start()

    def wait(cs):
        for c in cs:
            c.wait()

    def slot_of(step):
        return lax.rem(step, SLOTS)

    own = pltpu.make_async_copy(x_ref, xall.at[pl.ds(0, ROWS)], xsem)
    own.start()
    for s in range(SLOTS - 1):
        start(full(s, s))

    barrier = pltpu.get_barrier_semaphore()
    for other in (partner, remote):
        pl.semaphore_signal(barrier, inc=1, device_id=other, device_id_type=MESH)
    pl.semaphore_wait(barrier, 2)

    to_partner = pltpu.make_async_remote_copy(
        src_ref=x_ref, dst_ref=xall.at[pl.ds(ROWS, ROWS)],
        send_sem=px_send, recv_sem=px_recv,
        device_id=partner, device_id_type=MESH,
    )
    to_partner.start()

    def chunk(c):
        return pl.ds(pl.multiple_of(c * CW, CW), CW)

    def piece(c):
        return pl.ds(pl.multiple_of(c * NT, NT), NT)

    def gather_copy(c):
        return pltpu.make_async_remote_copy(
            src_ref=x_ref.at[:, piece(c)],
            dst_ref=xall.at[pl.ds(2 * ROWS, ROWS), piece(c)],
            send_sem=ag_send.at[c], recv_sem=ag_recv.at[c],
            device_id=remote, device_id_type=MESH,
        )

    def forward_copy(c):
        return pltpu.make_async_remote_copy(
            src_ref=xall.at[pl.ds(2 * ROWS, ROWS), piece(c)],
            dst_ref=xall.at[pl.ds(3 * ROWS, ROWS), piece(c)],
            send_sem=fw_send.at[c], recv_sem=fw_recv.at[c],
            device_id=partner, device_id_type=MESH,
        )

    @pl.loop(0, NX)
    def _(c):
        gather_copy(c).start()

    own.wait()
    to_partner.wait_recv()

    def forward(c):
        gather_copy(c).wait_recv()
        forward_copy(c).start()

    own_rows, far_rows = pl.ds(0, 2 * ROWS), pl.ds(2 * ROWS, 2 * ROWS)

    def dot(rows, ks, slot, j, at):
        return jnp.dot(
            xall[rows, ks], wbuf[slot, j, pl.ds(at, ks.size)], preferred_element_type=F32
        )

    def put(rows, t, g, u):
        hid[rows, pl.ds(pl.multiple_of(t * NT, NT), NT)] = (jax.nn.silu(g) * u).astype(BF16)

    def gate_up_own(t, slot):
        g, u = (dot(own_rows, pl.ds(0, D), slot, j, 0) for j in range(2))
        put(own_rows, t, g, u)

    def first_half(t, slot, tiles=2):
        for q in range(tiles):
            for j in range(2):
                acc[t + q, j] = dot(far_rows, pl.ds(0, HALF), slot, j, q * HALF)

    def second_half(t, slot, tiles=2):
        for q in range(tiles):
            g, u = (acc[t + q, j] + dot(far_rows, pl.ds(HALF, HALF), slot, j, q * HALF) for j in range(2))
            put(far_rows, t + q, g, u)

    def forward_at(k):
        @pl.loop(lax.div(5 * k + 1, 2) * jnp.minimum(k, 1), lax.div(5 * k + 6, 2))
        def _(c):
            forward(c)

    def arrived(lo, hi):
        @pl.loop(lo, hi)
        def _(c):
            forward_copy(c).wait_recv()

    def two_steps(i, work, ahead=None):
        s0, s1 = slot_of(i), slot_of(i + 1)
        wait(fetch(i))
        wait(fetch(i + 1))
        start(ahead[0] if ahead else fetch(i + 3))
        work(i, s0)
        start(ahead[1] if ahead else fetch(i + 4))
        work(i + 1, s1)

    @pl.loop(0, EARLY // 2)
    def _(k):
        two_steps(2 * k, gate_up_own)
        forward_at(k)

    arrived(0, NX // 2)

    @pl.loop(0, PAIRS // 2)
    def _(k):
        two_steps(S1 + 2 * k, lambda i, slot: first_half(2 * (i - S1), slot))
        forward_at(EARLY // 2 + k)

    wait(fetch(S2))
    start(fetch(S2 + 3))
    first_half(2 * PAIRS, S2 % SLOTS, 1)
    forward(NX - 1)

    wait(fetch(S2 + 1))
    start(fetch(S2 + 4))
    gate_up_own(EARLY, (S2 + 1) % SLOTS)
    arrived(NX // 2, NX)

    def second(i, slot):
        second_half(2 * (i - S3), slot)

    @pl.loop(0, PAIRS // 2 - 1)
    def _(k):
        two_steps(S3 + 2 * k, second)

    two_steps(S4 - 2, second, (tail((S4 + 1) % SLOTS), down(0, S5 % SLOTS)))
    wait(fetch(S4))
    start(down(1, (S5 + 1) % SLOTS))
    second_half(2 * PAIRS, S4 % SLOTS, 1)
    wait(tail((S4 + 1) % SLOTS))
    start(down(2, (S5 + 2) % SLOTS))
    for r in (far_rows, own_rows):
        gu = dot(r, pl.ds(0, D), (S4 + 1) % SLOTS, 0, 0)
        hid[r, pl.ds(NFULL * NT, TAIL)] = (
            jax.nn.silu(gu[:, :TAIL]) * gu[:, TAIL:]
        ).astype(BF16)

    def side_copy(src, dst, n, ssem, rsem, dev):
        return pltpu.make_async_remote_copy(
            src_ref=src, dst_ref=dst.at[n], send_sem=ssem.at[n], recv_sem=rsem.at[n],
            device_id=dev, device_id_type=MESH,
        )

    FAR = LATE + 2

    def turn(n):
        return lax.rem(n + NC - FAR, NC)

    def r_copy(n):
        return side_copy(send_r.at[lax.rem(n, 2)], recv_r, n, rr_send, rr_recv, partner)

    def l_copy(n):
        return side_copy(send_l.at[lax.rem(turn(n), 2)], recv_l, n, rl_send, rl_recv, partner)

    def x_copy(n):
        return side_copy(stage.at[n], recv_x, n, rx_send, rx_recv, remote)

    def y_copy(n):
        return pltpu.make_async_copy(stage.at[n], y_ref.at[:, chunk(n)], ysem.at[n])

    def term(rows, slot, j):
        return jnp.dot(hid[rows], wbuf[slot, j, pl.ds(0, FF)], preferred_element_type=F32)

    def ready_own(n):
        @pl.when(turn(n) >= 2)
        def _():
            l_copy(lax.rem(n + NC - 2, NC)).wait_send()

    def term_far(n, slot):
        for j in range(2):
            col = pl.ds(j * NT, NT)
            t = term(far_rows, slot, j)
            kept[lax.rem(n, 2), :, col] = t[:ROWS]
            send_r[lax.rem(n, 2), :, col] = t[ROWS:].astype(BF16)

    def term_own(n, slot):
        for j in range(2):
            t = term(own_rows, slot, j)
            acc[n, j, pl.ds(0, ROWS)] = t[:ROWS]
            send_l[lax.rem(turn(n), 2), :, pl.ds(j * NT, NT)] = t[ROWS:].astype(BF16)

    def reduce_far(n):
        r_copy(n).wait_recv()
        stage[n] = (kept[lax.rem(n, 2)] + recv_r[n].astype(F32)).astype(BF16)
        x_copy(n).start()

    def finish(n):
        l_copy(n).wait_recv()
        x_copy(n).wait()
        for j in range(2):
            col = pl.ds(j * NT, NT)
            stage[n, :, col] = (
                acc[n, j, pl.ds(0, ROWS)] + recv_l[n, :, col].astype(F32) + recv_x[n, :, col].astype(F32)
            ).astype(BF16)
        y_copy(n).start()

    wait(down(0, S5 % SLOTS))
    start(full(EARLY + 1, (S5 + 3) % SLOTS))
    term_far(0, S5 % SLOTS)
    r_copy(0).start()
    wait(down(1, (S5 + 1) % SLOTS))
    start(down(3, (S5 + 4) % SLOTS))
    term_far(1, (S5 + 1) % SLOTS)
    r_copy(1).start()
    reduce_far(0)

    @pl.loop(0, LATE)
    def _(k):
        s = S5 + 2 + 2 * k
        slot = slot_of(s)
        wait(down(k + 2, slot))

        @pl.when(k + 1 < LATE)
        def _():
            start(full(EARLY + k + 2, slot_of(s + 3)))

        @pl.when(k + 1 == LATE)
        def _():
            start(down(FAR + 1, slot_of(s + 3)))

        r_copy(k).wait_send()
        term_far(k + 2, slot)
        r_copy(k + 2).start()
        reduce_far(k + 1)
        slot = slot_of(s + 1)
        wait(full(EARLY + k + 1, slot))
        start(down(jnp.where(k + 1 < LATE, k + 4, FAR + 2), slot_of(s + 4)))
        gate_up_own(EARLY + k + 1, slot)

    reduce_far(FAR - 1)
    S6 = S5 + FAR + LATE

    @pl.loop(FAR, NC)
    def _(n):
        s = S6 + n - FAR
        slot = slot_of(s)
        wait(down(n, slot))
        start(down(lax.rem(n + 3, NC), slot_of(s + 3)))
        r_copy(n - 2).wait_send()
        ready_own(n)
        term_far(n, slot)
        term_own(n, slot)
        r_copy(n).start()
        l_copy(n).start()

        @pl.when(n > FAR)
        def _():
            reduce_far(n - 1)

    S7 = S6 + NC - FAR

    @pl.loop(0, FAR)
    def _(n):
        slot = slot_of(S7 + n)
        wait(down(n, slot))

        @pl.when(n + 3 < FAR)
        def _():
            start(down(n + 3, slot_of(S7 + n + 3)))

        ready_own(n)
        term_own(n, slot)
        l_copy(n).start()

        @pl.when(n == 0)
        def _():
            reduce_far(NC - 1)

        @pl.when(n > 0)
        def _():
            finish(FAR + n - 1)

    for n in range(2 * FAR - 1, NC - 1):
        finish(n)

    @pl.loop(0, FAR - 1)
    def _(n):
        finish(n)

    finish(NC - 1)
    finish(FAR - 1)

    for n in (NC - 2, NC - 1):
        r_copy(n).wait_send()
        l_copy((n + FAR) % NC).wait_send()
    to_partner.wait_send()

    @pl.loop(0, NX)
    def _(c):
        gather_copy(c).wait_send()
        forward_copy(c).wait_send()

    @pl.loop(0, NC)
    def _(n):
        y_copy(n).wait()


PARTS = 10


def settle(y_ref, out_ref, buf, isem, osem):
    rows = [pl.ds(i * (ROWS // PARTS), ROWS // PARTS) for i in range(PARTS)]
    ins = [pltpu.make_async_copy(y_ref.at[r], buf.at[r], isem.at[i]) for i, r in enumerate(rows)]
    outs = [pltpu.make_async_copy(buf.at[r], out_ref.at[r], osem.at[i]) for i, r in enumerate(rows)]
    for c in ins:
        c.start()
    for c, o in zip(ins, outs):
        c.wait()
        o.start()
    for o in outs:
        o.wait()


def solution(mesh):
    dma = pltpu.SemaphoreType.DMA

    def step(x, w_gate, w_up, w_down):
        y = pl.pallas_call(
            kernel,
            out_shape=jax.ShapeDtypeStruct((ROWS, D), BF16),
            in_specs=[pl.BlockSpec(memory_space=pl.ANY)] * 4,
            out_specs=pl.BlockSpec(memory_space=pl.ANY),
            scratch_shapes=[
                pltpu.VMEM((4 * ROWS, D), BF16),
                pltpu.VMEM((4 * ROWS, FF), BF16),
                pltpu.VMEM((SLOTS, 2, D, NT), BF16),
                pltpu.VMEM((NFULL, 2, 2 * ROWS, NT), F32),
                pltpu.VMEM((2, ROWS, CW), F32),
                pltpu.VMEM((2, ROWS, CW), BF16),
                pltpu.VMEM((NC, ROWS, CW), BF16),
                pltpu.VMEM((NC, ROWS, CW), BF16),
                pltpu.VMEM((NC, ROWS, CW), BF16),
                pltpu.VMEM((2, ROWS, CW), BF16),
                pltpu.VMEM((NC, ROWS, CW), BF16),
                dma, dma((SLOTS, 4)),
                dma((NX,)), dma((NX,)), dma((NX,)), dma((NX,)), dma, dma,
                dma((NC,)), dma((NC,)), dma((NC,)), dma((NC,)), dma((NC,)), dma((NC,)),
                dma((NC,)),
            ],
            compiler_params=pltpu.CompilerParams(
                collective_id=0, has_side_effects=True, vmem_limit_bytes=67043328
            ),
            cost_estimate=pl.CostEstimate(
                flops=6 * 4 * ROWS * D * FF, bytes_accessed=3 * D * FF * 2, transcendentals=4 * ROWS * FF
            ),
        )(x, w_gate, w_up, w_down)
        return pl.pallas_call(
            settle,
            out_shape=jax.ShapeDtypeStruct((ROWS, D), BF16),
            in_specs=[pl.BlockSpec(memory_space=pl.ANY)],
            out_specs=pl.BlockSpec(memory_space=pl.ANY),
            scratch_shapes=[pltpu.VMEM((ROWS, D), BF16), dma((PARTS,)), dma((PARTS,))],
        )(y)

    return jax.shard_map(
        step,
        mesh=mesh,
        in_specs=(P(("dp", "tp"), None), P(None, "tp"), P(None, "tp"), P("tp", None)),
        out_specs=P(("dp", "tp"), None),
        check_vma=False,
    )
```

```python
import functools

import jax
import jax.numpy as jnp
from jax import lax
from jax.experimental import pallas as pl
from jax.experimental.pallas import tpu as pltpu
from jax.sharding import PartitionSpec as P

MESH = pl.DeviceIdType.MESH
F32 = jnp.float32
BF16 = jnp.bfloat16

D = 6656
FF = 4480
ROWS = 160
NT = 256
NFULL = FF // NT
TAIL = FF - NFULL * NT
CW = 512
NC = D // CW
NX = D // NT
SLOTS = 4
HALF = D // 2
PAIRS = NFULL // 2
EARLY = 12
LATE = NFULL - EARLY - 1
S1 = EARLY
S2 = S1 + PAIRS
S3 = S2 + 2
S4 = S3 + PAIRS
S5 = S4 + 2


def kernel(
    x_ref, wg_ref, wu_ref, wd_ref, y_ref,
    xall, hid, wbuf, acc,
    kept, send_r, recv_r, stage, recv_x, send_l, recv_l,
    xsem, wsem,
    ag_send, ag_recv, fw_send, fw_recv, px_send, px_recv,
    rr_send, rr_recv, rx_send, rx_recv, rl_send, rl_recv, ysem,
):
    dp = lax.axis_index("dp")
    tp = lax.axis_index("tp")
    core = lax.rem(tp, 2)
    chip = lax.div(tp, 2)
    partner = (dp, chip * 2 + (1 - core))
    remote = (dp, (1 - chip) * 2 + core)

    def copies(parts, slot):
        return [
            pltpu.make_async_copy(src, wbuf.at[slot, j, pl.ds(row, src.shape[0]), pl.ds(c, src.shape[1])], wsem.at[slot, k])
            for k, (src, j, row, c) in enumerate(parts)
        ]

    def cols(ref, t):
        return ref.at[:, pl.ds(pl.multiple_of(t * NT, NT), NT)]

    def halves(pick, slot):
        parts = []
        for q in range(2):
            h, t = pick(q)
            row = pl.ds(pl.multiple_of(h * HALF, HALF), HALF)
            parts += [(cols(w.at[row], t), j, q * HALF, 0) for j, w in enumerate((wg_ref, wu_ref))]
        return copies(parts, slot)

    def full(t, slot):
        return halves(lambda q: (q, t), slot)

    def fetch(step):
        def pick(q):
            own = (step < S1) | (step == S3 - 1)
            p = step - jnp.where(step >= S3, S3, S1)
            h = jnp.where(own, q, jnp.where(step >= S3, 1, 0))
            t = jnp.where(own, jnp.minimum(step, EARLY), jnp.minimum(2 * p + q, NFULL - 1))
            return h, t

        return halves(pick, slot_of(step))

    def tail(slot):
        col = pl.ds(NFULL * NT, TAIL)
        return copies([(w.at[:, col], 0, 0, j * TAIL) for j, w in enumerate((wg_ref, wu_ref))], slot)

    def down(n, slot):
        return copies([(cols(wd_ref, 2 * n + j), j, 0, 0) for j in range(2)], slot)

    def start(cs):
        for c in cs:
            c.start()

    def wait(cs):
        for c in cs:
            c.wait()

    def slot_of(step):
        return lax.rem(step, SLOTS)

    own = pltpu.make_async_copy(x_ref, xall.at[pl.ds(0, ROWS)], xsem)
    own.start()
    for s in range(SLOTS - 1):
        start(full(s, s))

    barrier = pltpu.get_barrier_semaphore()
    for other in (partner, remote):
        pl.semaphore_signal(barrier, inc=1, device_id=other, device_id_type=MESH)
    pl.semaphore_wait(barrier, 2)

    to_partner = pltpu.make_async_remote_copy(
        src_ref=x_ref, dst_ref=xall.at[pl.ds(ROWS, ROWS)],
        send_sem=px_send, recv_sem=px_recv,
        device_id=partner, device_id_type=MESH,
    )
    to_partner.start()

    def chunk(c):
        return pl.ds(pl.multiple_of(c * CW, CW), CW)

    def piece(c):
        return pl.ds(pl.multiple_of(c * NT, NT), NT)

    def gather_copy(c):
        return pltpu.make_async_remote_copy(
            src_ref=x_ref.at[:, piece(c)],
            dst_ref=xall.at[pl.ds(2 * ROWS, ROWS), piece(c)],
            send_sem=ag_send.at[c], recv_sem=ag_recv.at[c],
            device_id=remote, device_id_type=MESH,
        )

    def forward_copy(c):
        return pltpu.make_async_remote_copy(
            src_ref=xall.at[pl.ds(2 * ROWS, ROWS), piece(c)],
            dst_ref=xall.at[pl.ds(3 * ROWS, ROWS), piece(c)],
            send_sem=fw_send.at[c], recv_sem=fw_recv.at[c],
            device_id=partner, device_id_type=MESH,
        )

    @pl.loop(0, NX)
    def _(c):
        gather_copy(c).start()

    def forward(c):
        gather_copy(c).wait_recv()
        forward_copy(c).start()

    own_rows, far_rows = pl.ds(0, 2 * ROWS), pl.ds(2 * ROWS, 2 * ROWS)

    def dot(rows, ks, slot, j, at):
        return jnp.dot(
            xall[rows, ks], wbuf[slot, j, pl.ds(at, ks.size)], preferred_element_type=F32
        )

    def put(rows, t, g, u):
        hid[rows, pl.ds(pl.multiple_of(t * NT, NT), NT)] = (jax.nn.silu(g) * u).astype(BF16)

    def gate_up_own(t, slot, rows=own_rows):
        g, u = (dot(rows, pl.ds(0, D), slot, j, 0) for j in range(2))
        put(rows, t, g, u)

    def first_half(t, slot, tiles=2):
        for q in range(tiles):
            for j in range(2):
                acc[t + q, j] = dot(far_rows, pl.ds(0, HALF), slot, j, q * HALF)

    def second_half(t, slot, tiles=2):
        for q in range(tiles):
            g, u = (acc[t + q, j] + dot(far_rows, pl.ds(HALF, HALF), slot, j, q * HALF) for j in range(2))
            put(far_rows, t + q, g, u)

    def forward_at(k):
        @pl.loop(lax.div(5 * k + 1, 2) * jnp.minimum(k, 1), lax.div(5 * k + 6, 2))
        def _(c):
            forward(c)

    def arrived(lo, hi):
        @pl.loop(lo, hi)
        def _(c):
            forward_copy(c).wait_recv()

    def two_steps(i, work, ahead=None):
        s0, s1 = slot_of(i), slot_of(i + 1)
        wait(fetch(i))
        wait(fetch(i + 1))
        start(ahead[0] if ahead else fetch(i + 3))
        work(i, s0)
        start(ahead[1] if ahead else fetch(i + 4))
        work(i + 1, s1)

    own.wait()
    wait(fetch(0))
    gate_up_own(0, 0, pl.ds(0, ROWS))
    to_partner.wait_recv()
    wait(fetch(1))
    start(fetch(3))
    gate_up_own(0, 0, pl.ds(ROWS, ROWS))
    start(fetch(4))
    gate_up_own(1, 1)
    for c in range(3):
        forward(c)

    @pl.loop(1, EARLY // 2)
    def _(k):
        two_steps(2 * k, gate_up_own)
        forward_at(k)

    arrived(0, NX // 2)

    @pl.loop(0, PAIRS // 2)
    def _(k):
        two_steps(S1 + 2 * k, lambda i, slot: first_half(2 * (i - S1), slot))
        forward_at(EARLY // 2 + k)

    wait(fetch(S2))
    start(fetch(S2 + 3))
    first_half(2 * PAIRS, S2 % SLOTS, 1)
    forward(NX - 1)

    wait(fetch(S2 + 1))
    start(fetch(S2 + 4))
    gate_up_own(EARLY, (S2 + 1) % SLOTS)
    arrived(NX // 2, NX)

    def second(i, slot):
        second_half(2 * (i - S3), slot)

    @pl.loop(0, PAIRS // 2 - 1)
    def _(k):
        two_steps(S3 + 2 * k, second)

    two_steps(S4 - 2, second, (tail((S4 + 1) % SLOTS), down(0, S5 % SLOTS)))
    wait(fetch(S4))
    wait(tail((S4 + 1) % SLOTS))
    start(down(1, (S5 + 1) % SLOTS))
    second_half(2 * PAIRS, S4 % SLOTS, 1)
    start(down(2, (S5 + 2) % SLOTS))
    for r in (far_rows, own_rows):
        gu = dot(r, pl.ds(0, D), (S4 + 1) % SLOTS, 0, 0)
        hid[r, pl.ds(NFULL * NT, TAIL)] = (
            jax.nn.silu(gu[:, :TAIL]) * gu[:, TAIL:]
        ).astype(BF16)

    def side_copy(src, dst, n, ssem, rsem, dev):
        return pltpu.make_async_remote_copy(
            src_ref=src, dst_ref=dst.at[n], send_sem=ssem.at[n], recv_sem=rsem.at[n],
            device_id=dev, device_id_type=MESH,
        )

    FAR = LATE + 2

    def turn(n):
        return lax.rem(n + NC - FAR, NC)

    def r_copy(n):
        return side_copy(send_r.at[lax.rem(n, 2)], recv_r, n, rr_send, rr_recv, partner)

    def l_copy(n):
        return side_copy(send_l.at[lax.rem(turn(n), 2)], recv_l, n, rl_send, rl_recv, partner)

    def x_copy(n):
        return side_copy(stage.at[n], recv_x, n, rx_send, rx_recv, remote)

    def y_copy(n):
        return pltpu.make_async_copy(stage.at[n], y_ref.at[:, chunk(n)], ysem.at[n])

    def term(rows, slot, j):
        return jnp.dot(hid[rows], wbuf[slot, j, pl.ds(0, FF)], preferred_element_type=F32)

    def ready_own(n):
        @pl.when(turn(n) >= 2)
        def _():
            l_copy(lax.rem(n + NC - 2, NC)).wait_send()

    def term_far(n, slot):
        for j in range(2):
            col = pl.ds(j * NT, NT)
            t = term(far_rows, slot, j)
            kept[lax.rem(n, 2), :, col] = t[:ROWS]
            send_r[lax.rem(n, 2), :, col] = t[ROWS:].astype(BF16)

    def term_own(n, slot):
        for j in range(2):
            t = term(own_rows, slot, j)
            acc[n, j, pl.ds(0, ROWS)] = t[:ROWS]
            send_l[lax.rem(turn(n), 2), :, pl.ds(j * NT, NT)] = t[ROWS:].astype(BF16)

    def reduce_far(n):
        r_copy(n).wait_recv()
        stage[n] = (kept[lax.rem(n, 2)] + recv_r[n].astype(F32)).astype(BF16)
        x_copy(n).start()

    def finish(n):
        l_copy(n).wait_recv()
        x_copy(n).wait()
        for j in range(2):
            col = pl.ds(j * NT, NT)
            stage[n, :, col] = (
                acc[n, j, pl.ds(0, ROWS)] + recv_l[n, :, col].astype(F32) + recv_x[n, :, col].astype(F32)
            ).astype(BF16)
        y_copy(n).start()

    wait(down(0, S5 % SLOTS))
    start(full(EARLY + 1, (S5 + 3) % SLOTS))
    term_far(0, S5 % SLOTS)
    r_copy(0).start()
    wait(down(1, (S5 + 1) % SLOTS))
    start(down(3, (S5 + 4) % SLOTS))
    term_far(1, (S5 + 1) % SLOTS)
    r_copy(1).start()
    reduce_far(0)

    @pl.loop(0, LATE)
    def _(k):
        s = S5 + 2 + 2 * k
        slot = slot_of(s)
        wait(down(k + 2, slot))

        @pl.when(k + 1 < LATE)
        def _():
            start(full(EARLY + k + 2, slot_of(s + 3)))

        @pl.when(k + 1 == LATE)
        def _():
            start(down(FAR + 1, slot_of(s + 3)))

        r_copy(k).wait_send()
        term_far(k + 2, slot)
        r_copy(k + 2).start()
        reduce_far(k + 1)
        slot = slot_of(s + 1)
        wait(full(EARLY + k + 1, slot))
        start(down(jnp.where(k + 1 < LATE, k + 4, FAR + 2), slot_of(s + 4)))
        gate_up_own(EARLY + k + 1, slot)

    reduce_far(FAR - 1)
    S6 = S5 + FAR + LATE

    @pl.loop(FAR, NC)
    def _(n):
        s = S6 + n - FAR
        slot = slot_of(s)
        wait(down(n, slot))
        start(down(lax.rem(n + 3, NC), slot_of(s + 3)))
        r_copy(n - 2).wait_send()
        ready_own(n)
        term_far(n, slot)
        term_own(n, slot)
        r_copy(n).start()
        l_copy(n).start()

        @pl.when(n > FAR)
        def _():
            reduce_far(n - 1)

    S7 = S6 + NC - FAR

    @pl.loop(0, FAR)
    def _(n):
        slot = slot_of(S7 + n)
        wait(down(n, slot))

        @pl.when(n + 3 < FAR)
        def _():
            start(down(n + 3, slot_of(S7 + n + 3)))

        ready_own(n)
        term_own(n, slot)
        l_copy(n).start()

        @pl.when(n == 0)
        def _():
            reduce_far(NC - 1)

        @pl.when(n > 0)
        def _():
            finish(FAR + n - 1)

    for n in range(2 * FAR - 1, NC - 1):
        finish(n)

    @pl.loop(0, FAR - 1)
    def _(n):
        finish(n)

    finish(NC - 1)
    finish(FAR - 1)

    for n in (NC - 2, NC - 1):
        r_copy(n).wait_send()
        l_copy((n + FAR) % NC).wait_send()
    to_partner.wait_send()

    @pl.loop(0, NX)
    def _(c):
        gather_copy(c).wait_send()
        forward_copy(c).wait_send()

    @pl.loop(0, NC)
    def _(n):
        y_copy(n).wait()


PARTS = 10


def settle(y_ref, out_ref, buf, isem, osem):
    rows = [pl.ds(i * (ROWS // PARTS), ROWS // PARTS) for i in range(PARTS)]
    ins = [pltpu.make_async_copy(y_ref.at[r], buf.at[r], isem.at[i]) for i, r in enumerate(rows)]
    outs = [pltpu.make_async_copy(buf.at[r], out_ref.at[r], osem.at[i]) for i, r in enumerate(rows)]
    for c in ins:
        c.start()
    for c, o in zip(ins, outs):
        c.wait()
        o.start()
    for o in outs:
        o.wait()


def solution(mesh):
    dma = pltpu.SemaphoreType.DMA

    def step(x, w_gate, w_up, w_down):
        y = pl.pallas_call(
            kernel,
            out_shape=jax.ShapeDtypeStruct((ROWS, D), BF16),
            in_specs=[pl.BlockSpec(memory_space=pl.ANY)] * 4,
            out_specs=pl.BlockSpec(memory_space=pl.ANY),
            scratch_shapes=[
                pltpu.VMEM((4 * ROWS, D), BF16),
                pltpu.VMEM((4 * ROWS, FF), BF16),
                pltpu.VMEM((SLOTS, 2, D, NT), BF16),
                pltpu.VMEM((NFULL, 2, 2 * ROWS, NT), F32),
                pltpu.VMEM((2, ROWS, CW), F32),
                pltpu.VMEM((2, ROWS, CW), BF16),
                pltpu.VMEM((NC, ROWS, CW), BF16),
                pltpu.VMEM((NC, ROWS, CW), BF16),
                pltpu.VMEM((NC, ROWS, CW), BF16),
                pltpu.VMEM((2, ROWS, CW), BF16),
                pltpu.VMEM((NC, ROWS, CW), BF16),
                dma, dma((SLOTS, 4)),
                dma((NX,)), dma((NX,)), dma((NX,)), dma((NX,)), dma, dma,
                dma((NC,)), dma((NC,)), dma((NC,)), dma((NC,)), dma((NC,)), dma((NC,)),
                dma((NC,)),
            ],
            compiler_params=pltpu.CompilerParams(
                collective_id=0, has_side_effects=True, vmem_limit_bytes=67043328
            ),
            cost_estimate=pl.CostEstimate(
                flops=6 * 4 * ROWS * D * FF, bytes_accessed=3 * D * FF * 2, transcendentals=4 * ROWS * FF
            ),
        )(x, w_gate, w_up, w_down)
        return pl.pallas_call(
            settle,
            out_shape=jax.ShapeDtypeStruct((ROWS, D), BF16),
            in_specs=[pl.BlockSpec(memory_space=pl.ANY)],
            out_specs=pl.BlockSpec(memory_space=pl.ANY),
            scratch_shapes=[pltpu.VMEM((ROWS, D), BF16), dma((PARTS,)), dma((PARTS,))],
        )(y)

    return jax.shard_map(
        step,
        mesh=mesh,
        in_specs=(P(("dp", "tp"), None), P(None, "tp"), P(None, "tp"), P("tp", None)),
        out_specs=P(("dp", "tp"), None),
        check_vma=False,
    )
```
